32 devices in a mesh: dp: 2 (over x), sp: 16 (over y, z, core).
Axes of the slice: x: 2, y: 2, z: 4, core: 2. Of those that a mesh axis runs over, the one named last changes fastest.
Arguments:
- q: bfloat16 [64, 32, 160], P('dp'), parts along dimension 0
- k: bfloat16 [64, 8192, 8, 160], P('dp', 'sp'), parts along dimension 0
- v: bfloat16 [64, 8192, 8, 160], P('dp', 'sp'), parts along dimension 0
Outputs:
- q: bfloat16 [64, 32, 160], P('dp'), parts along dimension 0
There are 2 independent parts. The reference program is written for one: setup_inputs(seed, part) draws one part's arguments, and reference() takes and returns one part's arrays. A program takes and returns all parts, laid end to end along the dimension named above; each array names one.
All inputs are finite; a program needn't handle non-finite values.
Results may differ from the reference program's by a relative error of at most 0.012.
Values are sent between devices in bfloat16 or wider.
A program may use at most 2 GiB of HBM per device.

```python
import jax
import jax.numpy as jnp

BATCH = 32
CACHE = 8192
HEADS = 32
KV_HEADS = 8
HEAD = 160


def setup_inputs(seed: int = 0, part: int = 0) -> dict:
    kq, kk, kv = (jax.random.fold_in(k, part) for k in jax.random.split(jax.random.key(seed), 3))
    return {
        "q": (3 * jax.random.normal(kq, (BATCH, HEADS, HEAD), jnp.float32)).astype(jnp.bfloat16),
        "k": jax.random.normal(kk, (BATCH, CACHE, KV_HEADS, HEAD), jnp.float32).astype(jnp.bfloat16),
        "v": jax.random.normal(kv, (BATCH, CACHE, KV_HEADS, HEAD), jnp.float32).astype(jnp.bfloat16),
    }


def einsum(form, a, b):
    return jnp.einsum(form, a.astype(jnp.float32), b.astype(jnp.float32))


def reference(q, k, v):
    grouped = q.reshape(BATCH, KV_HEADS, -1, HEAD)
    scores = einsum("bgsd,bugd->bgsu", grouped, k) * HEAD**-0.5
    weights = jax.nn.softmax(scores, -1).astype(jnp.bfloat16)
    return einsum("bgsu,bugd->bgsd", weights, v).astype(jnp.bfloat16).reshape(BATCH, HEADS, HEAD)
```

```python
import functools
import jax
import jax.numpy as jnp
from jax import lax
from jax.experimental import pallas as pl
from jax.experimental.pallas import tpu as pltpu
from jax.sharding import PartitionSpec as P

MESH = pl.DeviceIdType.MESH
SLOTS = 8
LAG = 5
LOG2E = 1.4426950408889634


def owner_of(i):
    r = i % 16
    far, core, z, y = r // 8, r // 4 % 2, r // 2 % 2, r % 2
    return y * 8 + (far * (1 + z) + (1 - far) * 3 * z) * 2 + core


def kernel(
    q_hbm, k_hbm, v_hbm, out, q_ref, kbuf, vbuf, qbd, s_scr, part, stat, parts, stats,
    qsem, ksem, vsem, part_send, stat_send, part_recv, stat_recv, out_send, out_recv,
):
    n_seq, wide, tokens = k_hbm.shape
    heads, head = q_hbm.shape[1:]
    groups = wide // head
    per = heads // groups
    scale = head**-0.5
    me = lax.axis_index("sp")
    n_dev = parts.shape[1]

    def kcopy(i, slot):
        return pltpu.make_async_copy(k_hbm.at[i], kbuf.at[slot], ksem.at[slot])

    def vcopy(i, slot):
        return pltpu.make_async_copy(v_hbm.at[i], vbuf.at[slot], vsem.at[slot])

    qcopy = pltpu.make_async_copy(q_hbm, q_ref, qsem)
    qcopy.start()
    for i in range(SLOTS):
        kcopy(i, i).start()
        vcopy(i, i).start()

    barrier = pltpu.get_barrier_semaphore()
    for d in range(1, n_dev):
        pl.semaphore_signal(barrier, inc=1, device_id={"sp": (me + d) % n_dev}, device_id_type=MESH)

    col = lax.broadcasted_iota(jnp.int32, (head, wide), 1)
    row = lax.broadcasted_iota(jnp.int32, (head, wide), 0)
    spread = jnp.where(lax.rem(col, head) == row, 1.0, 0.0).astype(jnp.bfloat16)
    step = 4
    own = lax.broadcasted_iota(jnp.int32, (heads, wide), 0) // per == lax.broadcasted_iota(jnp.int32, (heads, wide), 1) // head
    qcopy.wait()

    def spread_one(b, _):
        x = q_ref[pl.ds(b * step, step)].reshape(step * heads, head)
        y = jnp.dot(x, spread, preferred_element_type=jnp.float32)
        for s in range(step):
            qbd[b * step + s] = jnp.where(own, y[s * heads : (s + 1) * heads], 0.0).astype(jnp.bfloat16)
        return 0

    lax.fori_loop(0, n_seq // step, spread_one, 0)

    sub = lax.broadcasted_iota(jnp.int32, (8, head), 0) < per
    lane = lax.broadcasted_iota(jnp.int32, (heads, 128), 1)

    def scores(i, slot):
        return jnp.dot(qbd[i], kbuf[slot], preferred_element_type=jnp.float32)

    def values(i, slot, s):
        high = jnp.max(s, -1, keepdims=True)
        p = jnp.exp2((s - high) * (scale * LOG2E))
        total = jnp.sum(p, -1, keepdims=True)
        pb = p.astype(jnp.bfloat16)
        outs = []
        for j in range(heads // 16):
            half = pb[16 * j : 16 * j + 16]
            o = [
                lax.dot_general(half, vbuf[slot, pl.ds((4 * j + g) * head, head)], (((1,), (1,)), ((), ())), preferred_element_type=jnp.float32)
                for g in range(4)
            ]
            for t in range(2):
                outs.append(jnp.where(sub, o[2 * t][8 * t : 8 * t + 8], o[2 * t + 1][8 * t : 8 * t + 8]))
        part[i] = jnp.concatenate(outs, 0).astype(jnp.bfloat16)
        stat[i] = jnp.where(lane == 0, high * scale, total).T[:2, :heads]

    def part_copies(i, rd, to):
        return (
            pltpu.make_async_remote_copy(part.at[i], parts.at[rd, me], part_send, part_recv.at[rd], device_id={"sp": to}, device_id_type=MESH),
            pltpu.make_async_remote_copy(stat.at[i], stats.at[rd, me], stat_send, stat_recv.at[rd], device_id={"sp": to}, device_id_type=MESH),
        )

    def send(i, rd, to):
        @pl.when(to != me)
        def _():
            for copy in part_copies(i, rd, to):
                copy.start()

        @pl.when(to == me)
        def _():
            parts[rd, me] = part[i]
            stats[rd, me] = stat[i]

    def together(i, rd, to):
        @pl.when(to == me)
        def _():
            others = pl.ds(0, n_dev - 1)
            for ref, recv in ((parts, part_recv), (stats, stat_recv)):
                pltpu.make_async_remote_copy(ref.at[rd, others], ref.at[rd, others], part_send, recv.at[rd], device_id={"sp": me}, device_id_type=MESH).wait_recv()
            highs = [stats[rd, d, 0:1] for d in range(n_dev)]
            totals = [stats[rd, d, 1:2] for d in range(n_dev)]
            high = functools.reduce(jnp.maximum, highs)
            shares = [jnp.exp(h - high) for h in highs]
            total = functools.reduce(jnp.add, [a * b for a, b in zip(shares, totals)])
            shares = jnp.concatenate(shares, 0) / total
            shares = shares.T
            acc = None
            for d in range(n_dev):
                term = parts[rd, d].astype(jnp.float32) * shares[:, d : d + 1]
                acc = term if acc is None else acc + term
            out[i] = acc.astype(jnp.bfloat16)
            for d in range(1, n_dev):
                pltpu.make_async_remote_copy(out.at[i], out.at[i], out_send, out_recv, device_id={"sp": (me + d) % n_dev}, device_id_type=MESH).start()

    kcopy(0, 0).wait()
    s_scr[...] = scores(0, 0)
    kcopy(SLOTS, 0).start()
    pl.semaphore_wait(barrier, n_dev - 1)

    def trip(c, last):
        for j in range(SLOTS):
            i = c * SLOTS + j
            after = (j + 1) % SLOTS
            more = not (last and j == SLOTS - 1)
            if more:
                kcopy(i + 1, after).wait()
            vcopy(i, j).wait()
            s = s_scr[...]
            values(i, j, s)
            if more:
                s_scr[...] = scores(i + 1, after)
            if not last:
                vcopy(i + SLOTS, j).start()
                if j < SLOTS - 1:
                    kcopy(i + 1 + SLOTS, after).start()
                else:

                    @pl.when(c < n_seq // SLOTS - 2)
                    def _():
                        kcopy(i + 1 + SLOTS, after).start()

            def sent(e=i - 1):
                send(e, e // 16, owner_of(e))

            if j > 0 or last:
                sent()
            else:
                pl.when(c > 0)(sent)

            def joined(e=i - LAG):
                together(e, e // 16, owner_of(e))

            if j >= LAG or last:
                joined()
            else:
                pl.when(c > 0)(joined)

    def body(c, _):
        trip(c, False)
        return 0

    trips = n_seq // SLOTS
    lax.fori_loop(0, trips - 1, body, 0)
    trip(trips - 1, True)
    send(n_seq - 1, 1, owner_of(n_seq - 1))
    for e in range(n_seq - LAG, n_seq):
        together(e, 1, owner_of(e))

    count = pl.ds(0, n_seq - 2)
    everyone = {"device_id": {"sp": me}, "device_id_type": MESH}
    pltpu.make_async_remote_copy(part.at[count], part.at[count], part_send, out_recv, **everyone).wait_send()
    pltpu.make_async_remote_copy(stat.at[count], stat.at[count], stat_send, out_recv, **everyone).wait_send()
    finished = pltpu.make_async_remote_copy(out.at[count], out.at[count], out_send, out_recv, **everyone)
    finished.wait_send()
    finished.wait_recv()


def attend(q, k, v, n_dev):
    n, heads, head = q.shape
    tokens, groups = k.shape[1:3]
    wide = groups * head
    kt = k.transpose(0, 2, 3, 1).reshape(n, wide, tokens)
    vt = v.transpose(0, 2, 3, 1).reshape(n, wide, tokens)
    dma = pltpu.SemaphoreType.DMA
    return pl.pallas_call(
        kernel,
        out_shape=jax.ShapeDtypeStruct((n, heads, head), jnp.bfloat16),
        in_specs=[pl.BlockSpec(memory_space=pl.ANY)] * 3,
        out_specs=pl.BlockSpec(memory_space=pltpu.VMEM),
        scratch_shapes=[
            pltpu.VMEM((n, heads, head), jnp.bfloat16),
            pltpu.VMEM((SLOTS, wide, tokens), jnp.bfloat16),
            pltpu.VMEM((SLOTS, wide, tokens), jnp.bfloat16),
            pltpu.VMEM((n, heads, wide), jnp.bfloat16),
            pltpu.VMEM((heads, tokens), jnp.float32),
            pltpu.VMEM((n, heads, head), jnp.bfloat16),
            pltpu.VMEM((n, 2, heads), jnp.float32),
            pltpu.VMEM((2, n_dev, heads, head), jnp.bfloat16),
            pltpu.VMEM((2, n_dev, 2, heads), jnp.float32),
            dma(()), dma((SLOTS,)), dma((SLOTS,)), dma(()), dma(()), dma((2,)), dma((2,)), dma(()), dma(()),
        ],
        compiler_params=pltpu.CompilerParams(vmem_limit_bytes=60 * 1024 * 1024, collective_id=0, has_side_effects=True),
    )(q, kt, vt)


def solution(mesh):
    n_dev = mesh.shape["sp"]

    return jax.shard_map(
        lambda q, k, v: attend(q, k, v, n_dev),
        mesh=mesh,
        in_specs=(P("dp", None, None), P("dp", "sp", None, None), P("dp", "sp", None, None)),
        out_specs=P("dp", None, None),
        check_vma=False,
    )
```

```python
import functools
import jax
import jax.numpy as jnp
from jax import lax
from jax.experimental import pallas as pl
from jax.experimental.pallas import tpu as pltpu
from jax.sharding import PartitionSpec as P

MESH = pl.DeviceIdType.MESH
KAHEAD, VAHEAD = 3, 3
SLOTS = 8
PAIR, OWNER, HAND = 3, 12, 20
LOG2E = 1.4426950408889634


def chip_of(i):
    h = i // 2 % 8
    far, z, y = h // 4, h // 2 % 2, h % 2
    return y * 4 + far * (1 + z) + (1 - far) * 3 * z


def kernel(
    q_hbm, k_hbm, v_hbm, out, q_ref, kbuf, vbuf, s_scr, mine, theirs, part, stat, parts, stats,
    qsem, ksem, vsem, pair_send, pair_recv, part_send, stat_send, part_recv, stat_recv, out_send, out_recv, hand_send, hand_recv,
):
    n_seq, wide, tokens = k_hbm.shape
    heads, head = q_hbm.shape[1:]
    groups = wide // head
    per = heads // groups
    scale = head**-0.5
    me = lax.axis_index("sp")
    chip, core = me // 2, me % 2
    other = chip * 2 + 1 - core
    chips = parts.shape[1]
    tail = head - 128

    def remote(src, dst, send, recv, to):
        return pltpu.make_async_remote_copy(src, dst, send, recv, device_id={"sp": to}, device_id_type=MESH)

    def kcopy(i, slot):
        return pltpu.make_async_copy(k_hbm.at[i], kbuf.at[slot], ksem.at[slot])

    def vcopy(i, slot):
        return pltpu.make_async_copy(v_hbm.at[i], vbuf.at[slot], vsem.at[slot])

    qcopy = pltpu.make_async_copy(q_hbm, q_ref, qsem)
    qcopy.start()
    for i in range(KAHEAD + 1):
        kcopy(i, i).start()
        if i < VAHEAD:
            vcopy(i, i).start()

    barrier = pltpu.get_barrier_semaphore()
    for d in range(1, chips):
        pl.semaphore_signal(barrier, inc=1, device_id={"sp": (me + 2 * d) % (2 * chips)}, device_id_type=MESH)
    pl.semaphore_signal(barrier, inc=1, device_id={"sp": other}, device_id_type=MESH)

    row = lax.broadcasted_iota(jnp.int32, (16, tokens), 0) // per
    lane = lax.broadcasted_iota(jnp.int32, (heads, 128), 1)
    lane8 = lax.broadcasted_iota(jnp.int32, (8, 128), 1) // tail

    def only(x, g):
        return jnp.where(row[:, : x.shape[1]] == g, x, jnp.zeros_like(x))

    def scores(i, slot):
        halves = []
        for j in range(heads // 16):
            q = q_ref[i, 16 * j : 16 * j + 16]
            halves.append(
                sum(
                    jnp.dot(only(q, g), kbuf[slot, pl.ds((4 * j + g) * head, head)], preferred_element_type=jnp.float32)
                    for g in range(16 // per)
                )
            )
        return jnp.concatenate(halves, 0)

    def values(i, slot, s):
        high = jnp.max(s, -1, keepdims=True)
        p = jnp.exp2((s - high) * (scale * LOG2E))
        total = jnp.sum(p, -1, keepdims=True)
        pb = p.astype(jnp.bfloat16)
        mine[i, 1] = jnp.where(lane == 64, high * scale, total)
        for j in range(heads // 16):
            half = pb[16 * j : 16 * j + 16]
            o = sum(
                lax.dot_general(only(half, g), vbuf[slot, pl.ds((4 * j + g) * head, head)], (((1,), (1,)), ((), ())), preferred_element_type=jnp.float32)
                for g in range(16 // per)
            )
            mine[i, 0, 16 * j : 16 * j + 16] = o[:, :128]
            mine[i, 1, 16 * j : 16 * j + 16, :tail] = o[:, 128:]

    def pair_copy(i):
        return remote(mine.at[i], theirs.at[i // 2], pair_send, pair_recv.at[i // 2], other)

    def give(i):
        @pl.when(core != i % 2)
        def _():
            pair_copy(i).start()

    def pair(i):
        @pl.when(core == i % 2)
        def _():
            h, rd, to = i // 2, i // 16, chip_of(i)
            pair_copy(i).wait_recv()
            a0, a1, b0, b1 = mine[i, 0], mine[i, 1], theirs[h, 0], theirs[h, 1]
            ah, at, bh, bt = a1[:, 64:65], a1[:, 65:66], b1[:, 64:65], b1[:, 65:66]
            high = jnp.maximum(ah, bh)
            fa, fb = jnp.exp(ah - high), jnp.exp(bh - high)
            total = at * fa + bt * fb
            o0 = a0 * fa + b0 * fb
            o1 = a1 * fa + b1 * fb
            packed = o1[0:8]
            for j in range(1, heads // 8):
                packed = jnp.where(lane8 == j, pltpu.roll(o1[8 * j : 8 * j + 8], tail * j, 1), packed)
            part[h] = jnp.concatenate([o0, packed], 0).astype(jnp.bfloat16)
            stat[h] = jnp.where(lane == 0, high, total).T[:2, :heads]

            @pl.when(to != chip)
            def _():
                remote(part.at[h], parts.at[rd, chip], part_send, part_recv.at[rd], 2 * to + core).start()
                remote(stat.at[h], stats.at[rd, chip], stat_send, stat_recv.at[rd], 2 * to + core).start()

            @pl.when(to == chip)
            def _():
                parts[rd, chip] = part[h]
                stats[rd, chip] = stat[h]

    def together(i):
        rd = i // 16

        @pl.when(2 * chip_of(i) + i % 2 == me)
        def _():
            others = pl.ds(0, chips - 1)
            remote(parts.at[rd, others], parts.at[rd, others], part_send, part_recv.at[rd], other).wait_recv()
            remote(stats.at[rd, others], stats.at[rd, others], stat_send, stat_recv.at[rd], other).wait_recv()
            highs = [stats[rd, d, 0:1] for d in range(chips)]
            totals = [stats[rd, d, 1:2] for d in range(chips)]
            high = functools.reduce(jnp.maximum, highs)
            shares = [jnp.exp(h - high) for h in highs]
            total = functools.reduce(jnp.add, [a * b for a, b in zip(shares, totals)])
            shares = (jnp.concatenate(shares, 0) / total).T
            acc0 = acc1 = None
            for d in range(chips):
                share = jnp.broadcast_to(shares[:, d : d + 1], (heads, 128))
                packed = share[0:8]
                for j in range(1, heads // 8):
                    packed = jnp.where(lane8 == j, share[8 * j : 8 * j + 8], packed)
                x = parts[rd, d].astype(jnp.float32)
                t0, t1 = x[:heads] * share, x[heads:] * packed
                acc0, acc1 = (t0, t1) if d == 0 else (acc0 + t0, acc1 + t1)
            out[i, :, :128] = acc0.astype(jnp.bfloat16)
            rest = [acc1] + [pltpu.roll(acc1, 128 - tail * j, 1) for j in range(1, heads // 8)]
            out[i, :, 128:] = jnp.concatenate(rest, 0)[:, :tail].astype(jnp.bfloat16)
            for d in range(1, chips):
                remote(out.at[i], out.at[i], out_send, out_recv.at[i // 2], (me + 2 * d) % (2 * chips)).start()
            remote(out.at[i], out.at[i], hand_send, hand_recv, other).start()

    def hand(i):
        @pl.when((core == i % 2) & (chip_of(i) != chip))
        def _():
            remote(out.at[i], out.at[i], out_send, out_recv.at[i // 2], other).wait_recv()
            remote(out.at[i], out.at[i], hand_send, hand_recv, other).start()

    qcopy.wait()
    kcopy(0, 0).wait()
    s_scr[...] = scores(0, 0)

    def trip(c, last):
        for j in range(SLOTS):
            i = c * SLOTS + j
            after = (j + 1) % SLOTS
            more = not (last and j == SLOTS - 1)
            if not last or j + VAHEAD < SLOTS:
                vcopy(i + VAHEAD, (j + VAHEAD) % SLOTS).start()
            if not last or j + 1 + KAHEAD < SLOTS:
                kcopy(i + 1 + KAHEAD, (j + 1 + KAHEAD) % SLOTS).start()
            if more:
                kcopy(i + 1, after).wait()
            vcopy(i, j).wait()
            s = s_scr[...]
            if more:
                later = scores(i + 1, after)
            values(i, j, s)
            if more:
                s_scr[...] = later

            def at(lag, f, e):
                if last or j >= lag:
                    f(e)
                elif lag - j <= (n_seq // SLOTS - 2) * SLOTS:
                    pl.when(c >= -((j - lag) // SLOTS))(lambda: f(e))

            if j == 0:
                if not last:
                    pl.when(c == 0)(lambda: pl.semaphore_wait(barrier, chips))
            at(1, give, i - 1)
            at(PAIR, pair, i - PAIR)
            at(OWNER, together, i - OWNER)
            at(HAND, hand, i - HAND)

    def body(c, _):
        trip(c, False)
        return 0

    trips = n_seq // SLOTS
    lax.fori_loop(0, trips - 1, body, 0)
    trip(trips - 1, True)
    give(n_seq - 1)
    for i in range(n_seq - PAIR, n_seq):
        pair(i)
    late = [(i + OWNER, together, i) for i in range(n_seq - OWNER, n_seq)] + [(i + HAND, hand, i) for i in range(n_seq - HAND, n_seq)]
    for _, f, i in sorted(late, key=lambda x: x[0]):
        f(i)

    half = pl.ds(0, n_seq // 2)
    remote(mine.at[half], mine.at[half], pair_send, hand_recv, other).wait_send()
    sent = pl.ds(0, n_seq // 2 - 2)
    remote(part.at[sent], part.at[sent], part_send, hand_recv, other).wait_send()
    remote(stat.at[sent], stat.at[sent], stat_send, hand_recv, other).wait_send()
    sent = pl.ds(0, 2 * (chips - 1))
    remote(out.at[sent], out.at[sent], out_send, hand_recv, other).wait_send()
    handed = remote(out.at[half], out.at[half], hand_send, hand_recv, other)
    handed.wait_send()
    handed.wait_recv()


def attend(q, k, v, n_dev):
    n, heads, head = q.shape
    tokens, groups = k.shape[1:3]
    wide, chips = groups * head, n_dev // 2
    kt = k.transpose(0, 2, 3, 1).reshape(n, wide, tokens)
    vt = v.transpose(0, 2, 3, 1).reshape(n, wide, tokens)
    dma = pltpu.SemaphoreType.DMA
    packed = heads + heads * (head - 128) // 128
    return pl.pallas_call(
        kernel,
        out_shape=pltpu.VMEM((n, heads, head), jnp.bfloat16),
        in_specs=[pl.BlockSpec(memory_space=pltpu.HBM)] * 3,
        out_specs=pl.BlockSpec(memory_space=pltpu.VMEM),
        scratch_shapes=[
            pltpu.VMEM((n, heads, head), jnp.bfloat16),
            pltpu.VMEM((SLOTS, wide, tokens), jnp.bfloat16),
            pltpu.VMEM((SLOTS, wide, tokens), jnp.bfloat16),
            pltpu.VMEM((heads, tokens), jnp.float32),
            pltpu.VMEM((n, 2, heads, 128), jnp.float32),
            pltpu.VMEM((n // 2, 2, heads, 128), jnp.float32),
            pltpu.VMEM((n // 2, packed, 128), jnp.bfloat16),
            pltpu.VMEM((n // 2, 2, heads), jnp.float32),
            pltpu.VMEM((2, chips, packed, 128), jnp.bfloat16),
            pltpu.VMEM((2, chips, 2, heads), jnp.float32),
            dma(()), dma((SLOTS,)), dma((SLOTS,)), dma(()), dma((n // 2,)), dma(()), dma(()), dma((2,)), dma((2,)),
            dma(()), dma((n // 2,)), dma(()), dma(()),
        ],
        compiler_params=pltpu.CompilerParams(vmem_limit_bytes=60 * 1024 * 1024, collective_id=0, has_side_effects=True),
    )(q, kt, vt)


def solution(mesh):
    n_dev = mesh.shape["sp"]

    return jax.shard_map(
        lambda q, k, v: attend(q, k, v, n_dev),
        mesh=mesh,
        in_specs=(P("dp", None, None), P("dp", "sp", None, None), P("dp", "sp", None, None)),
        out_specs=P("dp", None, None),
        check_vma=False,
    )
```

```python
import functools
import jax
import jax.numpy as jnp
from jax import lax
from jax.experimental import pallas as pl
from jax.experimental.pallas import tpu as pltpu
from jax.sharding import PartitionSpec as P

MESH = pl.DeviceIdType.MESH
AHEAD, LESS = 3, 3
LATE = 2
LAST = 4
SLOTS = 8
PAIR, OWNER, HAND = 3, 12, 20
LOG2E = 1.4426950408889634


def chip_of(i):
    h = i // 2 % 8
    far, z, y = h // 4, h // 2 % 2, h % 2
    return y * 4 + far * (1 + z) + (1 - far) * 3 * z


def kernel(
    q_hbm, k_hbm, v_hbm, out, q_ref, kbuf, vbuf, s_scr, mine, theirs, part, stat, parts, stats, all_parts, all_stats,
    qsem, ksem, vsem, pair_send, pair_recv, part_send, stat_send, part_recv, stat_recv, out_send, out_recv, hand_send, hand_recv, all_send, all_recv,
):
    n_seq, wide, tokens = k_hbm.shape
    heads, head = q_hbm.shape[1:]
    groups = wide // head
    per = heads // groups
    scale = head**-0.5
    me = lax.axis_index("sp")
    chip, core = me // 2, me % 2
    other = chip * 2 + 1 - core
    chips = parts.shape[1]
    tail = head - 128
    owned = n_seq - LAST

    def remote(src, dst, send, recv, to):
        return pltpu.make_async_remote_copy(src, dst, send, recv, device_id={"sp": to}, device_id_type=MESH)

    def kcopy(i, slot):
        return pltpu.make_async_copy(k_hbm.at[i], kbuf.at[slot], ksem.at[slot])

    def vcopy(i, slot):
        return pltpu.make_async_copy(v_hbm.at[i], vbuf.at[slot], vsem.at[slot])

    first, rest = (
        pltpu.make_async_copy(q_hbm.at[part_of_q], q_ref.at[part_of_q], qsem.at[x])
        for x, part_of_q in enumerate((pl.ds(0, SLOTS), pl.ds(SLOTS, n_seq - SLOTS)))
    )
    first.start()
    for i in range(AHEAD):
        kcopy(i, i).start()
        vcopy(i, i).start()
    rest.start()
    kcopy(AHEAD, AHEAD).start()

    barrier = pltpu.get_barrier_semaphore()
    for d in range(1, chips):
        pl.semaphore_signal(barrier, inc=1, device_id={"sp": (me + 2 * d) % (2 * chips)}, device_id_type=MESH)
    pl.semaphore_signal(barrier, inc=1, device_id={"sp": other}, device_id_type=MESH)

    row = lax.broadcasted_iota(jnp.int32, (16, tokens), 0) // per
    lane = lax.broadcasted_iota(jnp.int32, (heads, 128), 1)
    lane8 = lax.broadcasted_iota(jnp.int32, (8, 128), 1) // tail

    def only(x, g):
        return jnp.where(row[:, : x.shape[1]] == g, x, jnp.zeros_like(x))

    def scores(i, slot):
        halves = []
        for j in range(heads // 16):
            q = q_ref[i, 16 * j : 16 * j + 16]
            halves.append(
                sum(
                    jnp.dot(only(q, g), kbuf[slot, pl.ds((4 * j + g) * head, head)], preferred_element_type=jnp.float32)
                    for g in range(16 // per)
                )
            )
        return jnp.concatenate(halves, 0)

    def values(i, slot, s):
        high = jnp.max(s, -1, keepdims=True)
        p = jnp.exp2((s - high) * (scale * LOG2E))
        total = jnp.sum(p, -1, keepdims=True)
        pb = p.astype(jnp.bfloat16)
        mine[i, 1] = jnp.where(lane == 64, high * scale, total)
        for j in range(heads // 16):
            half = pb[16 * j : 16 * j + 16]
            o = sum(
                lax.dot_general(only(half, g), vbuf[slot, pl.ds((4 * j + g) * head, head)], (((1,), (1,)), ((), ())), preferred_element_type=jnp.float32)
                for g in range(16 // per)
            )
            mine[i, 0, 16 * j : 16 * j + 16] = o[:, :128]
            mine[i, 1, 16 * j : 16 * j + 16, :tail] = o[:, 128:]

    def pair_copy(i):
        return remote(mine.at[i], theirs.at[i // 2], pair_send, pair_recv.at[i // 2], other)

    def give(i):
        @pl.when(core != i % 2)
        def _():
            pair_copy(i).start()

    def pair(i):
        @pl.when(core == i % 2)
        def _():
            h, rd, to = i // 2, i // 16, chip_of(i)
            pair_copy(i).wait_recv()
            a0, a1, b0, b1 = mine[i, 0], mine[i, 1], theirs[h, 0], theirs[h, 1]
            ah, at, bh, bt = a1[:, 64:65], a1[:, 65:66], b1[:, 64:65], b1[:, 65:66]
            high = jnp.maximum(ah, bh)
            fa, fb = jnp.exp(ah - high), jnp.exp(bh - high)
            total = at * fa + bt * fb
            o0 = a0 * fa + b0 * fb
            o1 = a1 * fa + b1 * fb
            packed = o1[0:8]
            for j in range(1, heads // 8):
                packed = jnp.where(lane8 == j, pltpu.roll(o1[8 * j : 8 * j + 8], tail * j, 1), packed)
            part[h] = jnp.concatenate([o0, packed], 0).astype(jnp.bfloat16)

            if isinstance(i, int) and i >= owned:
                slot = h - (n_seq - LAST) // 2
                peers = [(me + 2 * d) % (2 * chips) for d in range(1, chips)]
                for peer in peers:
                    remote(part.at[h], all_parts.at[slot, chip], all_send.at[0], all_recv.at[slot, 0], peer).start()
                stat[h] = jnp.where(lane == 0, high, total).T[:2, :heads]
                for peer in peers:
                    remote(stat.at[h], all_stats.at[slot, chip], all_send.at[1], all_recv.at[slot, 1], peer).start()
                all_parts[slot, chip] = part[h]
                all_stats[slot, chip] = stat[h]
                return

            stat[h] = jnp.where(lane == 0, high, total).T[:2, :heads]

            @pl.when(to != chip)
            def _():
                remote(part.at[h], parts.at[rd, chip], part_send, part_recv.at[rd], 2 * to + core).start()
                remote(stat.at[h], stats.at[rd, chip], stat_send, stat_recv.at[rd], 2 * to + core).start()

            @pl.when(to == chip)
            def _():
                parts[rd, chip] = part[h]
                stats[rd, chip] = stat[h]

    def result(i, parts, stats, recv_part, recv_stat):
        others = pl.ds(0, chips - 1)
        remote(parts.at[others], parts.at[others], part_send, recv_part, other).wait_recv()
        remote(stats.at[others], stats.at[others], stat_send, recv_stat, other).wait_recv()
        highs = [stats[d, 0:1] for d in range(chips)]
        totals = [stats[d, 1:2] for d in range(chips)]
        high = functools.reduce(jnp.maximum, highs)
        shares = [jnp.exp(h - high) for h in highs]
        total = functools.reduce(jnp.add, [a * b for a, b in zip(shares, totals)])
        shares = (jnp.concatenate(shares, 0) / total).T
        acc0 = acc1 = None
        for d in range(chips):
            share = jnp.broadcast_to(shares[:, d : d + 1], (heads, 128))
            packed = share[0:8]
            for j in range(1, heads // 8):
                packed = jnp.where(lane8 == j, share[8 * j : 8 * j + 8], packed)
            x = parts[d].astype(jnp.float32)
            t0, t1 = x[:heads] * share, x[heads:] * packed
            acc0, acc1 = (t0, t1) if d == 0 else (acc0 + t0, acc1 + t1)
        out[i, :, :128] = acc0.astype(jnp.bfloat16)
        rest = [acc1] + [pltpu.roll(acc1, 128 - tail * j, 1) for j in range(1, heads // 8)]
        out[i, :, 128:] = jnp.concatenate(rest, 0)[:, :tail].astype(jnp.bfloat16)
        remote(out.at[i], out.at[i], hand_send, hand_recv, other).start()

    def together(i):
        rd = i // 16

        @pl.when(2 * chip_of(i) + i % 2 == me)
        def _():
            result(i, parts.at[rd], stats.at[rd], part_recv.at[rd], stat_recv.at[rd])
            for d in range(1, chips):
                remote(out.at[i], out.at[i], out_send, out_recv.at[i // 2], (me + 2 * d) % (2 * chips)).start()

    def everywhere(i):
        slot = i // 2 - (n_seq - LAST) // 2

        @pl.when(core == i % 2)
        def _():
            result(i, all_parts.at[slot], all_stats.at[slot], all_recv.at[slot, 0], all_recv.at[slot, 1])

    def hand(i):
        @pl.when((core == i % 2) & (chip_of(i) != chip))
        def _():
            remote(out.at[i], out.at[i], out_send, out_recv.at[i // 2], other).wait_recv()
            remote(out.at[i], out.at[i], hand_send, hand_recv, other).start()

    first.wait()
    kcopy(0, 0).wait()
    s_scr[...] = scores(0, 0)

    start = n_seq - SLOTS
    done = [start - 1, start - PAIR, start - OWNER, start - HAND]

    def lags(j):
        return 0, LATE, OWNER - min(j // 2, 2), HAND - min(j // 2, 2)

    def trip(c, last):
        for j in range(SLOTS):
            i = c * SLOTS + j
            after = (j + 1) % SLOTS
            more = not (last and j == SLOTS - 1)
            ahead = LESS if last else AHEAD
            if not last or AHEAD <= j + ahead < SLOTS:
                vcopy(i + ahead, (j + ahead) % SLOTS).start()
            if not last or AHEAD < j + 1 + ahead < SLOTS:
                kcopy(i + 1 + ahead, (j + 1 + ahead) % SLOTS).start()
            if not last and j == SLOTS - 2:
                pl.when(c == 0)(rest.wait)
            if more:
                kcopy(i + 1, after).wait()
            vcopy(i, j).wait()
            s = s_scr[...]
            if more:
                later = scores(i + 1, after)
            values(i, j, s)
            if more:
                s_scr[...] = later

            def at(lag, f, e):
                if last or j >= lag:
                    f(e)
                elif lag - j <= (n_seq // SLOTS - 2) * SLOTS:
                    pl.when(c >= -((j - lag) // SLOTS))(lambda: f(e))

            if j == 0:
                if not last:
                    pl.when(c == 0)(lambda: pl.semaphore_wait(barrier, chips))
            if not last:
                at(1, give, i - 1)
                at(PAIR, pair, i - PAIR)
                at(OWNER, together, i - OWNER)
                at(HAND, hand, i - HAND)
                continue
            for kind, f in enumerate((give, pair, together, hand)):
                for e in range(done[kind], i - lags(j)[kind] + 1):
                    f(e)
                    done[kind] = e + 1

    def body(c, _):
        trip(c, False)
        return 0

    trips = n_seq // SLOTS
    lax.fori_loop(0, trips - 1, body, 0)
    trip(trips - 1, True)
    for i in range(done[1], n_seq):
        pair(i)
    for i in range(done[2], owned):
        together(i)
    for i in range(owned, n_seq - 2):
        everywhere(i)
    for i in range(done[3], owned - 2):
        hand(i)
    for i in range(n_seq - 2, n_seq):
        everywhere(i)
    for i in range(owned - 2, owned):
        hand(i)

    half = pl.ds(0, n_seq // 2)
    remote(mine.at[half], mine.at[half], pair_send, hand_recv, other).wait_send()
    fewer = functools.reduce(jnp.logical_or, [chip_of(i) == chip for i in range(owned, n_seq, 2)])
    sent = pl.ds(0, owned // 2 - 2)
    one = pl.ds(0, 1)
    some = pl.ds(0, chips - 1)
    for ref, sem in ((part, part_send), (stat, stat_send)):
        remote(ref.at[sent], ref.at[sent], sem, hand_recv, other).wait_send()
        pl.when(fewer)(remote(ref.at[one], ref.at[one], sem, hand_recv, other).wait_send)
    for _ in range(LAST // 2):
        remote(part.at[some], part.at[some], all_send.at[0], hand_recv, other).wait_send()
        remote(stat.at[some], stat.at[some], all_send.at[1], hand_recv, other).wait_send()
    remote(out.at[some], out.at[some], out_send, hand_recv, other).wait_send()
    pl.when(jnp.logical_not(fewer))(remote(out.at[some], out.at[some], out_send, hand_recv, other).wait_send)
    handed = remote(out.at[half], out.at[half], hand_send, hand_recv, other)
    handed.wait_send()
    handed.wait_recv()


def attend(q, k, v, n_dev):
    n, heads, head = q.shape
    tokens, groups = k.shape[1:3]
    wide, chips = groups * head, n_dev // 2
    kt = k.transpose(0, 2, 3, 1).reshape(n, wide, tokens)
    vt = v.transpose(0, 2, 3, 1).reshape(n, wide, tokens)
    dma = pltpu.SemaphoreType.DMA
    packed = heads + heads * (head - 128) // 128
    return pl.pallas_call(
        kernel,
        out_shape=pltpu.VMEM((n, heads, head), jnp.bfloat16),
        in_specs=[pl.BlockSpec(memory_space=pltpu.HBM)] * 3,
        out_specs=pl.BlockSpec(memory_space=pltpu.VMEM),
        scratch_shapes=[
            pltpu.VMEM((n, heads, head), jnp.bfloat16),
            pltpu.VMEM((SLOTS, wide, tokens), jnp.bfloat16),
            pltpu.VMEM((SLOTS, wide, tokens), jnp.bfloat16),
            pltpu.VMEM((heads, tokens), jnp.float32),
            pltpu.VMEM((n, 2, heads, 128), jnp.float32),
            pltpu.VMEM((n // 2, 2, heads, 128), jnp.float32),
            pltpu.VMEM((n // 2, packed, 128), jnp.bfloat16),
            pltpu.VMEM((n // 2, 2, heads), jnp.float32),
            pltpu.VMEM((2, chips, packed, 128), jnp.bfloat16),
            pltpu.VMEM((2, chips, 2, heads), jnp.float32),
            pltpu.VMEM((LAST // 2, chips, packed, 128), jnp.bfloat16),
            pltpu.VMEM((LAST // 2, chips, 2, heads), jnp.float32),
            dma((2,)), dma((SLOTS,)), dma((SLOTS,)), dma(()), dma((n // 2,)), dma(()), dma(()), dma((2,)), dma((2,)),
            dma(()), dma((n // 2,)), dma(()), dma(()), dma((2,)), dma((LAST // 2, 2)),
        ],
        compiler_params=pltpu.CompilerParams(vmem_limit_bytes=60 * 1024 * 1024, collective_id=0, has_side_effects=True),
    )(q, kt, vt)


def solution(mesh):
    n_dev = mesh.shape["sp"]

    return jax.shard_map(
        lambda q, k, v: attend(q, k, v, n_dev),
        mesh=mesh,
        in_specs=(P("dp", None, None), P("dp", "sp", None, None), P("dp", "sp", None, None)),
        out_specs=P("dp", None, None),
        check_vma=False,
    )
```

```python
import functools
import jax
import jax.numpy as jnp
from jax import lax
from jax.experimental import pallas as pl
from jax.experimental.pallas import tpu as pltpu
from jax.sharding import PartitionSpec as P

MESH = pl.DeviceIdType.MESH
AHEAD, LESS = 3, 3
LATE = 2
LAST = 2
SLOTS = 8
PAIR, OWNER, HAND = 3, 12, 20
LOG2E = 1.4426950408889634


def chip_of(i):
    h = i // 2 % 8
    far, z, y = h // 4, h // 2 % 2, h % 2
    return y * 4 + far * (1 + z) + (1 - far) * 3 * z


def kernel(
    q_hbm, k_hbm, v_hbm, out, q_ref, kbuf, vbuf, s_scr, mine, theirs, part, stat, parts, stats, all_parts, all_stats,
    qsem, ksem, vsem, pair_send, pair_recv, part_send, stat_send, part_recv, stat_recv, out_send, out_recv, hand_send, hand_recv, all_send, all_recv,
):
    n_seq, wide, tokens = k_hbm.shape
    heads, head = q_hbm.shape[1:]
    groups = wide // head
    per = heads // groups
    scale = head**-0.5
    me = lax.axis_index("sp")
    chip, core = me // 2, me % 2
    other = chip * 2 + 1 - core
    chips = parts.shape[1]
    tail = head - 128
    owned = n_seq - LAST
    peers = [2 * (d + (d + chips - chip) // chips) + core for d in range(chips - 1)]

    def remote(src, dst, send, recv, to):
        return pltpu.make_async_remote_copy(src, dst, send, recv, device_id={"sp": to}, device_id_type=MESH)

    def kcopy(i, slot):
        return pltpu.make_async_copy(k_hbm.at[i], kbuf.at[slot], ksem.at[slot])

    def vcopy(i, slot):
        return pltpu.make_async_copy(v_hbm.at[i], vbuf.at[slot], vsem.at[slot])

    first, rest = (
        pltpu.make_async_copy(q_hbm.at[part_of_q], q_ref.at[part_of_q], qsem.at[x])
        for x, part_of_q in enumerate((pl.ds(0, SLOTS), pl.ds(SLOTS, n_seq - SLOTS)))
    )
    first.start()
    for i in range(AHEAD):
        kcopy(i, i).start()
        vcopy(i, i).start()
    rest.start()
    kcopy(AHEAD, AHEAD).start()

    barrier = pltpu.get_barrier_semaphore()
    for d in range(1, chips):
        pl.semaphore_signal(barrier, inc=1, device_id={"sp": (me + 2 * d) % (2 * chips)}, device_id_type=MESH)
    pl.semaphore_signal(barrier, inc=1, device_id={"sp": other}, device_id_type=MESH)

    row = lax.broadcasted_iota(jnp.int32, (16, tokens), 0) // per
    lane = lax.broadcasted_iota(jnp.int32, (heads, 128), 1)
    lane8 = lax.broadcasted_iota(jnp.int32, (8, 128), 1) // tail

    def only(x, g):
        return jnp.where(row[:, : x.shape[1]] == g, x, jnp.zeros_like(x))

    def scores(i, slot):
        halves = []
        for j in range(heads // 16):
            q = q_ref[i, 16 * j : 16 * j + 16]
            halves.append(
                sum(
                    jnp.dot(only(q, g), kbuf[slot, pl.ds((4 * j + g) * head, head)], preferred_element_type=jnp.float32)
                    for g in range(16 // per)
                )
            )
        return jnp.concatenate(halves, 0)

    def values(i, slot, s):
        high = jnp.max(s, -1, keepdims=True)
        p = jnp.exp2((s - high) * (scale * LOG2E))
        total = jnp.sum(p, -1, keepdims=True)
        pb = p.astype(jnp.bfloat16)
        mine[i, 1] = jnp.where(lane == 64, high * scale, total)
        for j in range(heads // 16):
            half = pb[16 * j : 16 * j + 16]
            o = sum(
                lax.dot_general(only(half, g), vbuf[slot, pl.ds((4 * j + g) * head, head)], (((1,), (1,)), ((), ())), preferred_element_type=jnp.float32)
                for g in range(16 // per)
            )
            mine[i, 0, 16 * j : 16 * j + 16] = o[:, :128]
            mine[i, 1, 16 * j : 16 * j + 16, :tail] = o[:, 128:]

    def pair_copy(i):
        return remote(mine.at[i], theirs.at[i // 2], pair_send, pair_recv.at[i // 2], other)

    def give(i):
        @pl.when(core != i % 2)
        def _():
            pair_copy(i).start()

    def pair(i):
        @pl.when(core == i % 2)
        def _():
            h, rd, to = i // 2, i // 16, chip_of(i)
            pair_copy(i).wait_recv()
            a0, a1, b0, b1 = mine[i, 0], mine[i, 1], theirs[h, 0], theirs[h, 1]
            ah, at, bh, bt = a1[:, 64:65], a1[:, 65:66], b1[:, 64:65], b1[:, 65:66]
            high = jnp.maximum(ah, bh)
            fa, fb = jnp.exp(ah - high), jnp.exp(bh - high)
            total = at * fa + bt * fb
            o0 = a0 * fa + b0 * fb
            o1 = a1 * fa + b1 * fb
            packed = o1[0:8]
            for j in range(1, heads // 8):
                packed = jnp.where(lane8 == j, pltpu.roll(o1[8 * j : 8 * j + 8], tail * j, 1), packed)
            part[h] = jnp.concatenate([o0, packed], 0).astype(jnp.bfloat16)

            if isinstance(i, int) and i >= owned:
                slot = h - (n_seq - LAST) // 2
                stat[h] = jnp.where(lane == 0, high, total).T[:2, :heads]
                for peer in peers:
                    remote(part.at[h], all_parts.at[slot, chip], all_send.at[0], all_recv.at[slot, 0], peer).start()
                    remote(stat.at[h], all_stats.at[slot, chip], all_send.at[1], all_recv.at[slot, 1], peer).start()
                all_parts[slot, chip] = part[h]
                all_stats[slot, chip] = stat[h]
                return

            stat[h] = jnp.where(lane == 0, high, total).T[:2, :heads]

            @pl.when(to != chip)
            def _():
                remote(part.at[h], parts.at[rd, chip], part_send, part_recv.at[rd], 2 * to + core).start()
                remote(stat.at[h], stats.at[rd, chip], stat_send, stat_recv.at[rd], 2 * to + core).start()

            @pl.when(to == chip)
            def _():
                parts[rd, chip] = part[h]
                stats[rd, chip] = stat[h]

    def result(i, parts, stats, recv_part, recv_stat):
        others = pl.ds(0, chips - 1)
        remote(parts.at[others], parts.at[others], part_send, recv_part, other).wait_recv()
        remote(stats.at[others], stats.at[others], stat_send, recv_stat, other).wait_recv()
        highs = [stats[d, 0:1] for d in range(chips)]
        totals = [stats[d, 1:2] for d in range(chips)]
        high = functools.reduce(jnp.maximum, highs)
        shares = [jnp.exp(h - high) for h in highs]
        total = functools.reduce(jnp.add, [a * b for a, b in zip(shares, totals)])
        shares = (jnp.concatenate(shares, 0) / total).T
        acc0 = acc1 = None
        for d in range(chips):
            share = jnp.broadcast_to(shares[:, d : d + 1], (heads, 128))
            packed = share[0:8]
            for j in range(1, heads // 8):
                packed = jnp.where(lane8 == j, share[8 * j : 8 * j + 8], packed)
            x = parts[d].astype(jnp.float32)
            t0, t1 = x[:heads] * share, x[heads:] * packed
            acc0, acc1 = (t0, t1) if d == 0 else (acc0 + t0, acc1 + t1)
        out[i, :, :128] = acc0.astype(jnp.bfloat16)
        rest = [acc1] + [pltpu.roll(acc1, 128 - tail * j, 1) for j in range(1, heads // 8)]
        out[i, :, 128:] = jnp.concatenate(rest, 0)[:, :tail].astype(jnp.bfloat16)
        remote(out.at[i], out.at[i], hand_send, hand_recv, other).start()

    def together(i):
        rd = i // 16

        @pl.when(2 * chip_of(i) + i % 2 == me)
        def _():
            result(i, parts.at[rd], stats.at[rd], part_recv.at[rd], stat_recv.at[rd])
            for peer in peers:
                remote(out.at[i], out.at[i], out_send, out_recv.at[i // 2], peer).start()

    def everywhere(i):
        slot = i // 2 - (n_seq - LAST) // 2

        @pl.when(core == i % 2)
        def _():
            result(i, all_parts.at[slot], all_stats.at[slot], all_recv.at[slot, 0], all_recv.at[slot, 1])

    def hand(i):
        @pl.when((core == i % 2) & (chip_of(i) != chip))
        def _():
            remote(out.at[i], out.at[i], out_send, out_recv.at[i // 2], other).wait_recv()
            remote(out.at[i], out.at[i], hand_send, hand_recv, other).start()

    first.wait()
    kcopy(0, 0).wait()
    s_scr[...] = scores(0, 0)

    start = n_seq - SLOTS
    done = [start - 1, start - PAIR, start - OWNER, start - HAND]

    def lags(j):
        return 0, LATE, OWNER - min(j // 2, 2), HAND - min(j // 2, 2)

    def trip(c, last):
        for j in range(SLOTS):
            i = c * SLOTS + j
            after = (j + 1) % SLOTS
            more = not (last and j == SLOTS - 1)
            ahead = LESS if last else AHEAD
            if not last or AHEAD <= j + ahead < SLOTS:
                vcopy(i + ahead, (j + ahead) % SLOTS).start()
            if not last or AHEAD < j + 1 + ahead < SLOTS:
                kcopy(i + 1 + ahead, (j + 1 + ahead) % SLOTS).start()
            if not last and j == SLOTS - 2:
                pl.when(c == 0)(rest.wait)
            if more:
                kcopy(i + 1, after).wait()
            vcopy(i, j).wait()
            s = s_scr[...]
            if more:
                later = scores(i + 1, after)
            values(i, j, s)
            if more:
                s_scr[...] = later

            def at(lag, f, e):
                if last or j >= lag:
                    f(e)
                elif lag - j <= (n_seq // SLOTS - 2) * SLOTS:
                    pl.when(c >= -((j - lag) // SLOTS))(lambda: f(e))

            if j == 0:
                if not last:
                    pl.when(c == 0)(lambda: pl.semaphore_wait(barrier, chips))
            if not last:
                at(1, give, i - 1)
                at(PAIR, pair, i - PAIR)
                at(OWNER, together, i - OWNER)
                at(HAND, hand, i - HAND)
                continue
            for kind, f in enumerate((give, pair, together, hand)):
                for e in range(done[kind], i - lags(j)[kind] + 1):
                    f(e)
                    done[kind] = e + 1

    def body(c, _):
        trip(c, False)
        return 0

    trips = n_seq // SLOTS
    lax.fori_loop(0, trips - 1, body, 0)
    trip(trips - 1, True)
    for i in range(done[1], n_seq):
        pair(i)
    for i in range(done[2], owned):
        together(i)
    for i in range(done[3], owned - 2):
        hand(i)
    for i in range(n_seq - 2, n_seq):
        everywhere(i)
    for i in range(owned - 2, owned):
        hand(i)

    half = pl.ds(0, n_seq // 2)
    remote(mine.at[half], mine.at[half], pair_send, hand_recv, other).wait_send()
    fewer = functools.reduce(jnp.logical_or, [chip_of(i) == chip for i in range(owned, n_seq, 2)])
    sent = pl.ds(0, owned // 2 - 2)
    one = pl.ds(0, 1)
    some = pl.ds(0, chips - 1)
    for ref, sem in ((part, part_send), (stat, stat_send)):
        remote(ref.at[sent], ref.at[sent], sem, hand_recv, other).wait_send()
        pl.when(fewer)(remote(ref.at[one], ref.at[one], sem, hand_recv, other).wait_send)
    for _ in range(LAST // 2):
        remote(part.at[some], part.at[some], all_send.at[0], hand_recv, other).wait_send()
        remote(stat.at[some], stat.at[some], all_send.at[1], hand_recv, other).wait_send()
    remote(out.at[some], out.at[some], out_send, hand_recv, other).wait_send()
    pl.when(jnp.logical_not(fewer))(remote(out.at[some], out.at[some], out_send, hand_recv, other).wait_send)
    handed = remote(out.at[half], out.at[half], hand_send, hand_recv, other)
    handed.wait_send()
    handed.wait_recv()


def attend(q, k, v, n_dev):
    n, heads, head = q.shape
    tokens, groups = k.shape[1:3]
    wide, chips = groups * head, n_dev // 2
    kt = k.transpose(0, 2, 3, 1).reshape(n, wide, tokens)
    vt = v.transpose(0, 2, 3, 1).reshape(n, wide, tokens)
    dma = pltpu.SemaphoreType.DMA
    packed = heads + heads * (head - 128) // 128
    return pl.pallas_call(
        kernel,
        out_shape=pltpu.VMEM((n, heads, head), jnp.bfloat16),
        in_specs=[pl.BlockSpec(memory_space=pltpu.HBM)] * 3,
        out_specs=pl.BlockSpec(memory_space=pltpu.VMEM),
        scratch_shapes=[
            pltpu.VMEM((n, heads, head), jnp.bfloat16),
            pltpu.VMEM((SLOTS, wide, tokens), jnp.bfloat16),
            pltpu.VMEM((SLOTS, wide, tokens), jnp.bfloat16),
            pltpu.VMEM((heads, tokens), jnp.float32),
            pltpu.VMEM((n, 2, heads, 128), jnp.float32),
            pltpu.VMEM((n // 2, 2, heads, 128), jnp.float32),
            pltpu.VMEM((n // 2, packed, 128), jnp.bfloat16),
            pltpu.VMEM((n // 2, 2, heads), jnp.float32),
            pltpu.VMEM((2, chips, packed, 128), jnp.bfloat16),
            pltpu.VMEM((2, chips, 2, heads), jnp.float32),
            pltpu.VMEM((LAST // 2, chips, packed, 128), jnp.bfloat16),
            pltpu.VMEM((LAST // 2, chips, 2, heads), jnp.float32),
            dma((2,)), dma((SLOTS,)), dma((SLOTS,)), dma(()), dma((n // 2,)), dma(()), dma(()), dma((2,)), dma((2,)),
            dma(()), dma((n // 2,)), dma(()), dma(()), dma((2,)), dma((LAST // 2, 2)),
        ],
        compiler_params=pltpu.CompilerParams(vmem_limit_bytes=60 * 1024 * 1024, collective_id=0, has_side_effects=True),
    )(q, kt, vt)


def solution(mesh):
    n_dev = mesh.shape["sp"]

    return jax.shard_map(
        lambda q, k, v: attend(q, k, v, n_dev),
        mesh=mesh,
        in_specs=(P("dp", None, None), P("dp", "sp", None, None), P("dp", "sp", None, None)),
        out_specs=P("dp", None, None),
        check_vma=False,
    )
```
